32 devices in a mesh: dp: 8 (over z, x), mp: 4 (over y, core).
Axes of the slice: x: 2, y: 2, z: 4, core: 2. Of those that a mesh axis runs over, the one named last changes fastest.
Arguments:
- activations: bfloat16 [1024, 1024], P('dp'), may hold values from -6 to 6
- cotangents: bfloat16 [1024, 4096], P('dp', 'mp'), may hold values from -1200 to 1200
- owners: int32 [4], replicated, may hold values from 0 to 7, as said below
Outputs:
- update: bfloat16 [1024, 4096], P('dp', 'mp')
- roots: float32 [4096, 2048], P('dp', 'mp')
- graft: float32 [], replicated
The draws below stay inside these ranges and needn't reach their ends.
Inputs may be any that keep to these rules, and one draw needn't show every extreme that they name: The left root of block b is computed at dp index owners[b] and its right root at owners[b] with its lowest bit flipped; every dp index computes exactly one root.
All inputs are finite; a program needn't handle non-finite values.
Results may differ from the reference program's by a relative error of at most 0.00045.
Values may be sent and summed in bfloat16 or wider, within the bound.
No kernel may reach another device: no remote copies, remote signals or barrier semaphores. Data moves between devices by JAX's collectives and lax.ppermute only.
A program may use at most 64 MiB of HBM per device.

```python
import math
import jax
import jax.numpy as jnp
from jax import lax

B = 512
CB = 2
ITERS = 3
RB = 2
NB = 4
DIN = 1024
DOUT = 4096
TOKENS = 1024
N_DP = 8
N_MP = 4


def draw_owners(key, part):
    pair_key = jax.random.fold_in(key, 11)
    side_key = jax.random.fold_in(key, 23)
    pairs = jax.random.permutation(pair_key, NB)
    sides = jax.random.randint(side_key, (NB,), 0, 2)
    return (2 * pairs + sides).astype(jnp.int32)


def draw_cotangents(key, part):
    base_key = jax.random.fold_in(key, 31)
    group_key = jax.random.fold_in(key, 37)
    pick_key = jax.random.fold_in(key, 41)
    base = jax.random.truncated_normal(base_key, -6.0, 6.0, (TOKENS, DOUT), jnp.float32)
    group_ids = jnp.arange(N_MP, dtype=jnp.int32)
    chosen = jax.random.randint(pick_key, (), 0, N_MP)
    group_scale = jnp.exp(jax.random.uniform(group_key, (N_MP,), jnp.float32, jnp.log(0.5), jnp.log(2.0)))
    group_scale = jnp.where(group_ids == chosen, 6.0, group_scale)
    column_scale = jnp.repeat(group_scale, CB * B)
    return (base * column_scale[None, :]).astype(jnp.bfloat16)


def block_levels(rng, dims, split, least, high):
    factor_of = 1.0
    for position, blocks in split:
        draws = jax.random.uniform(jax.random.fold_in(jax.random.fold_in(rng, 6), position), (blocks,), jnp.float32, least / len(split), high / len(split))
        factor_of = factor_of * jnp.repeat(jnp.exp(draws), dims[position] // blocks).reshape((-1,) + (1,) * (len(dims) - 1 - position))
    return factor_of


def normal_values(rng, shape, spread, most, pieces=(), kind=jnp.bfloat16):
    array = spread * jax.random.normal(rng, shape, jnp.float32)
    if pieces:
        array = array * block_levels(rng, shape, pieces, -0.22, 0.18)
    return jnp.clip(array, -most, most).astype(kind)


def setup_inputs(seed: int = 0) -> dict:
    splits = jax.random.split(jax.random.key(seed), 4)
    return {
        "activations": normal_values(splits[0], (TOKENS, DIN), 1.0, 6.0, ((0, 8),)),
        "cotangents": draw_cotangents(jax.random.fold_in(splits[3], 71), 0),
        "owners": draw_owners(jax.random.fold_in(splits[3], 71), 0),
    }


def product(left, right):
    return jnp.dot(left, right, precision=lax.Precision.HIGHEST, preferred_element_type=jnp.float32)

def statistic_of(operand):
    gram = product(operand, operand.T)
    ridge = 0.1 * (jnp.sum(operand * operand) / operand.shape[0] + 1.0)
    return gram + ridge * jnp.eye(operand.shape[0], dtype=jnp.float32)

def inverse_root(statistic):
    eye_matrix = jnp.eye(statistic.shape[0], dtype=jnp.float32)
    magnitude = jnp.sqrt(jnp.sum(statistic * statistic))
    current = statistic / magnitude
    result = eye_matrix
    for step in range(ITERS):
        factor = (5.0 * eye_matrix - current) * 0.25
        if step == 0:
            result = factor * magnitude ** (-0.25)
        else:
            result = product(result, factor)
        if step + 1 < ITERS:
            square = product(factor, factor)
            current = product(product(square, square), current)
    return result

def one_block(grad_block):
    left_root = inverse_root(statistic_of(grad_block))
    right_root = inverse_root(statistic_of(grad_block.T))
    precond = product(left_root, product(grad_block, right_root))
    return (left_root, right_root, precond)

def reference(activations, cotangents, owners):
    gradient = jnp.dot(activations.astype(jnp.float32).T, cotangents.astype(jnp.float32), precision=lax.Precision.HIGHEST, preferred_element_type=jnp.float32) / math.sqrt(TOKENS)
    columns_all = N_MP * CB
    blocks = gradient.reshape(RB, B, columns_all, B).transpose(0, 2, 1, 3).reshape(RB * columns_all, B, B)
    left_all, right_all, precond_all = lax.map(one_block, blocks)
    grad_total = jnp.sum(gradient * gradient)
    precond_total = jnp.sum(precond_all * precond_all)
    graft = jnp.sqrt(grad_total / jnp.maximum(precond_total, 1.0))
    whole = precond_all.reshape(RB, columns_all, B, B).transpose(0, 2, 1, 3).reshape(DIN, DOUT)
    update = (graft * whole).astype(jnp.bfloat16)
    index_dp = jnp.arange(N_DP, dtype=jnp.int32)
    partner = owners + 1 - 2 * (owners % 2)
    left_match = owners[None, :] == index_dp[:, None]
    right_match = partner[None, :] == index_dp[:, None]
    block_ids = jnp.arange(NB, dtype=jnp.int32)
    owned = lax.optimization_barrier(jnp.sum(jnp.where(left_match | right_match, block_ids[None, :], 0), axis=1)).astype(jnp.int32)
    is_left = jnp.any(left_match, axis=1)
    row_block = owned // CB
    col_block = owned % CB
    column_ids = jnp.arange(N_MP, dtype=jnp.int32)[None, :] * CB + col_block[:, None]
    flat_ids = (row_block[:, None] * columns_all + column_ids).astype(jnp.int32)
    picked = jnp.where(is_left[:, None, None, None], left_all[flat_ids], right_all[flat_ids])
    roots = picked.transpose(0, 2, 1, 3).reshape(N_DP * B, N_MP * B)
    return (update, roots, graft)
```

```python
import math

import jax
import jax.numpy as jnp
from jax import lax
from jax.experimental import pallas as pl
from jax.experimental.pallas import tpu as pltpu
from jax.sharding import PartitionSpec as P

B = 512
CB = 2
ITERS = 3
F32 = jnp.float32
BF16 = jnp.bfloat16
SMEM = pl.BlockSpec(memory_space=pltpu.SMEM)
VMEM = pl.BlockSpec(memory_space=pltpu.VMEM)


def block_of_pair(owners, block_count, pair):
    block = jnp.int32(0)
    for b in range(block_count):
        block = jnp.where(owners[b] // 2 == pair, b, block)
    return block


def pack_kernel(pairs, block_count, index, owners, activations, cotangents, *outs):
    pair = index[0] // 2
    for shift in range(pairs):
        block = block_of_pair(owners, block_count, (pair + shift) % pairs)
        row = pl.multiple_of(block // CB * B, B)
        col = pl.multiple_of(block % CB * B, B)
        outs[shift][0] = activations[:, pl.ds(row, B)]
        outs[shift][1] = cotangents[:, pl.ds(col, B)]


def mm(left, right):
    return jnp.dot(left, right, preferred_element_type=F32)


def mm_nt(left, right):
    return lax.dot_general(left, right, (((1,), (1,)), ((), ())), preferred_element_type=F32)


def halves(value):
    high = value.astype(BF16)
    return high, (value - high.astype(F32)).astype(BF16)


def mm_split(left, right):
    left_high, left_low = left
    right_high, right_low = right
    return mm(left_high, right_high) + (mm(left_high, right_low) + mm(left_low, right_high))


def raised(quarter):
    q = quarter.astype(BF16)
    rest = mm(q, q) - 2.5 * quarter
    d = rest.astype(BF16)
    rest = 3.125 * rest + mm(d, d)
    return 2.44140625 * quarter + mm(rest.astype(BF16), q)


def root_parts(gram, ridge, eye):
    statistic = gram + jnp.where(eye, ridge, 0.0)
    magnitude = jnp.sqrt(jnp.sum(statistic * statistic, keepdims=True))
    e1 = statistic * (0.25 / magnitude)
    e2 = raised(e1)
    e3 = raised(e2)
    rest = 1.25 * (e1 + e2) - mm(e1.astype(BF16), e2.astype(BF16))
    rest = 1.5625 * e3 + 1.25 * rest - mm(rest.astype(BF16), e3.astype(BF16))
    return 1.0 / jnp.sqrt(jnp.sqrt(magnitude)), rest


def root_kernel(pairs, block_count, piece_rows, index, owners, *refs):
    chunks = refs[: 2 * pairs]
    root_ref, sums_ref = refs[2 * pairs : 2 * pairs + 2]
    pieces = refs[2 * pairs + 2 : 3 * pairs + 2]
    a_ref, c_ref, g_ref, w_ref, l_ref, p_ref = refs[3 * pairs + 2 :]
    pair = index[0] // 2
    side = index[0] % 2
    block = block_of_pair(owners, block_count, pair)
    tokens = chunks[0].shape[1]
    for k, chunk in enumerate(chunks):
        a_ref[k * tokens : (k + 1) * tokens, :] = chunk[0]
        c_ref[k * tokens : (k + 1) * tokens, :] = chunk[1]
    gradient = lax.dot_general(
        a_ref[...], c_ref[...], (((0,), (0,)), ((), ())), preferred_element_type=F32
    ) * (1.0 / math.sqrt(tokens * 2 * pairs))
    g_ref[...] = gradient
    high, low = halves(gradient)
    high_t, low_t = high.T, low.T
    ridge = 0.1 * (jnp.sum(gradient * gradient, keepdims=True) / B + 1.0)
    eye = lax.broadcasted_iota(jnp.int32, (B, B), 0) == lax.broadcasted_iota(jnp.int32, (B, B), 1)
    left_gram = mm(high, high_t) + (mm(high, low_t) + mm(low, high_t))
    right_gram = mm(high_t, high) + (mm(high_t, low) + mm(low_t, high))
    left_scale, left_rest = root_parts(left_gram, ridge, eye)
    right_scale, right_rest = root_parts(right_gram, ridge, eye)
    is_left = owners[block] == index[0]

    @pl.when(is_left)
    def _():
        root_ref[...] = left_scale * (jnp.where(eye, 1.953125, 0.0) - left_rest)

    @pl.when(jnp.logical_not(is_left))
    def _():
        root_ref[...] = right_scale * (jnp.where(eye, 1.953125, 0.0) - right_rest)

    right_product = right_scale * (1.953125 * gradient - mm_split((high, low), halves(right_rest)))
    w_ref[...] = right_product
    l_ref[...] = left_rest
    count = B // piece_rows // 2
    starts = [pl.multiple_of((2 * k + side) * piece_rows, piece_rows) for k in range(count)]
    left_rows = jnp.concatenate([l_ref[pl.ds(s, piece_rows), :] for s in starts], axis=0)
    w_rows = jnp.concatenate([w_ref[pl.ds(s, piece_rows), :] for s in starts], axis=0)
    g_rows = jnp.concatenate([g_ref[pl.ds(s, piece_rows), :] for s in starts], axis=0)
    precond = left_scale * (1.953125 * w_rows - mm_split(halves(left_rows), halves(right_product)))
    p_ref[...] = precond.reshape(count, piece_rows, B)

    def lanes(value):
        total = jnp.sum(value * value, axis=0, keepdims=True)
        return sum(total[:, i : i + 128] for i in range(0, B, 128))

    row_ids = lax.broadcasted_iota(jnp.int32, (8, 128), 0)
    sums_ref[...] = jnp.where(row_ids == 0, lanes(g_rows), jnp.where(row_ids == 1, lanes(precond), 0.0))
    for shift in range(pairs):
        want = (pair + shift) % pairs - block // CB * count
        pieces[shift][...] = p_ref[jnp.clip(want, 0, count - 1)]


def finish_kernel(pairs, block_count, piece_rows, index, owners, sums, *refs):
    pieces = refs[:pairs]
    update_ref, graft_ref = refs[pairs:]
    pair = index[0] // 2
    count = B // piece_rows // 2
    grad_total = jnp.sum(sums[0:1, :], keepdims=True)
    precond_total = jnp.sum(sums[1:2, :], keepdims=True)
    graft = jnp.sqrt(grad_total / jnp.maximum(precond_total, 1.0))
    graft_ref[...] = graft
    for c in range(CB):
        source = owners[pair // count * CB + c] // 2
        shift = (pair - source + pairs) % pairs
        for k in range(pairs):

            @pl.when(shift == k)
            def _(k=k, c=c):
                update_ref[:, c * B : (c + 1) * B] = (graft * pieces[k][...]).astype(BF16)


def summed_over(value, axis):
    size = lax.axis_size(axis)
    bit = 1
    while bit < size:
        value = value + lax.ppermute(value, axis, [(i, i ^ bit) for i in range(size)])
        bit *= 2
    return value


def on_device(activations, cotangents, owners):
    dp_count = lax.axis_size("dp")
    pairs = dp_count // 2
    block_count = owners.shape[0]
    local_tokens, features = activations.shape
    piece_rows = features // dp_count
    index = lax.axis_index("dp").astype(jnp.int32).reshape(1)
    chunk_type = jax.ShapeDtypeStruct((2, local_tokens, B), BF16)
    packed = pl.pallas_call(
        lambda *refs: pack_kernel(pairs, block_count, *refs),
        out_shape=[chunk_type] * pairs,
        in_specs=[SMEM, SMEM, VMEM, VMEM],
        out_specs=[VMEM] * pairs,
    )(index, owners, activations, cotangents)

    def along(value, shift):
        return lax.ppermute(value, "dp", [(i, (i + 2 * shift) % dp_count) for i in range(dp_count)])

    def across(value):
        return lax.ppermute(value, "dp", [(i, i ^ 1) for i in range(dp_count)])

    mine = [packed[0]] + [along(packed[s], s) for s in range(1, pairs)]
    other = [across(chunk) for chunk in mine]
    all_tokens = local_tokens * dp_count
    piece_type = jax.ShapeDtypeStruct((piece_rows, B), F32)
    root, sums, *pieces = pl.pallas_call(
        lambda *refs: root_kernel(pairs, block_count, piece_rows, *refs),
        out_shape=[jax.ShapeDtypeStruct((B, B), F32), jax.ShapeDtypeStruct((8, 128), F32)]
        + [piece_type] * pairs,
        in_specs=[SMEM, SMEM] + [VMEM] * (2 * pairs),
        out_specs=[VMEM] * (pairs + 2),
        scratch_shapes=[
            pltpu.VMEM((all_tokens, B), BF16),
            pltpu.VMEM((all_tokens, B), BF16),
            pltpu.VMEM((B, B), F32),
            pltpu.VMEM((B, B), F32),
            pltpu.VMEM((B, B), F32),
            pltpu.VMEM((B // piece_rows // 2, piece_rows, B), F32),
        ],
    )(index, owners, *mine, *other)
    totals = summed_over(summed_over(sums, "mp"), "dp")
    arrived = [pieces[0]] + [along(pieces[s], s) for s in range(1, pairs)]
    update, graft = pl.pallas_call(
        lambda *refs: finish_kernel(pairs, block_count, piece_rows, *refs),
        out_shape=[
            jax.ShapeDtypeStruct((piece_rows, CB * B), BF16),
            jax.ShapeDtypeStruct((1, 1), F32),
        ],
        in_specs=[SMEM, SMEM] + [VMEM] * (pairs + 1),
        out_specs=[VMEM, VMEM],
    )(index, owners, totals, *arrived)
    return (update, root, graft.reshape(()))


def solution(mesh):
    return jax.shard_map(
        on_device,
        mesh=mesh,
        in_specs=(P("dp", None), P("dp", "mp"), P()),
        out_specs=(P("dp", "mp"), P("dp", "mp"), P()),
        check_vma=False,
    )
```

```python
import math

import jax
import jax.numpy as jnp
from jax import lax
from jax.experimental import pallas as pl
from jax.experimental.pallas import tpu as pltpu
from jax.sharding import PartitionSpec as P


B = 512
CB = 2
F32 = jnp.float32
BF16 = jnp.bfloat16
SMEM = pl.BlockSpec(memory_space=pltpu.SMEM)
VMEM = pl.BlockSpec(memory_space=pltpu.VMEM)


def block_of_pair(owners, block_count, pair):
    block = jnp.int32(0)
    for b in range(block_count):
        block = jnp.where(owners[b] // 2 == pair, b, block)
    return block


def pack_kernel(pairs, block_count, index, owners, activations, cotangents, *outs):
    pair = index[0] // 2
    part_rows = outs[0].shape[0]
    first = pl.multiple_of(index[1] * part_rows, part_rows)
    for shift in range(pairs):
        block = block_of_pair(owners, block_count, (pair + shift) % pairs)
        row = pl.multiple_of(block // CB * B, B)
        col = pl.multiple_of(block % CB * B, B)
        outs[shift][...] = activations[pl.ds(first, part_rows), pl.ds(row, B)]
        outs[pairs + shift][...] = cotangents[:, pl.ds(col, B)]


def mm(left, right):
    return jnp.dot(left, right, preferred_element_type=F32)


def halves(value):
    high = value.astype(BF16)
    return high, (value - high.astype(F32)).astype(BF16)


def mm_split(left, right):
    left_high, left_low = left
    right_high, right_low = right
    return mm(left_high, right_high) + (mm(left_high, right_low) + mm(left_low, right_high))


def raised(quarter):
    q = quarter.astype(BF16)
    rest = mm(q, q) - 2.5 * quarter
    d = rest.astype(BF16)
    rest = 3.125 * rest + mm(d, d)
    return 2.44140625 * quarter + mm(rest.astype(BF16), q)


def root_parts(gram, ridge, eye):
    statistic = gram + jnp.where(eye, ridge, 0.0)
    magnitude = jnp.sqrt(jnp.sum(statistic * statistic, keepdims=True))
    e1 = statistic * (0.25 / magnitude)
    e2 = raised(e1)
    e3 = raised(e2)
    rest = 1.25 * (e1 + e2) - mm(e1.astype(BF16), e2.astype(BF16))
    rest = 1.5625 * e3 + 1.25 * rest - mm(rest.astype(BF16), e3.astype(BF16))
    return 1.0 / jnp.sqrt(jnp.sqrt(magnitude)), rest


def root_kernel(pairs, parts, block_count, piece_rows, index, owners, *refs):
    token_parts, refs = refs[:parts], refs[parts:]
    chunks = refs[: 2 * pairs]
    root_ref, sums_ref = refs[2 * pairs : 2 * pairs + 2]
    pieces = refs[2 * pairs + 2 : 3 * pairs + 2]
    a_ref, c_ref, g_ref, w_ref, l_ref, p_ref = refs[3 * pairs + 2 :]
    pair = index[0] // 2
    side = index[0] % 2
    block = block_of_pair(owners, block_count, pair)
    tokens = chunks[0].shape[0]
    part_rows = tokens // parts
    for k, chunk in enumerate(chunks):
        c_ref[k * tokens : (k + 1) * tokens, :] = chunk[...]
        for m, part in enumerate(token_parts):
            start = pl.multiple_of(k * tokens + (index[1] ^ m) * part_rows, part_rows)
            a_ref[pl.ds(start, part_rows), :] = part[k * part_rows : (k + 1) * part_rows, :]
    gradient = lax.dot_general(
        a_ref[...], c_ref[...], (((0,), (0,)), ((), ())), preferred_element_type=F32
    ) * (1.0 / math.sqrt(tokens * 2 * pairs))
    g_ref[...] = gradient
    high, low = halves(gradient)
    high_t, low_t = high.T, low.T
    ridge = 0.1 * (jnp.sum(gradient * gradient, keepdims=True) / B + 1.0)
    eye = lax.broadcasted_iota(jnp.int32, (B, B), 0) == lax.broadcasted_iota(jnp.int32, (B, B), 1)
    left_gram = mm(high, high_t) + (mm(high, low_t) + mm(low, high_t))
    right_gram = mm(high_t, high) + (mm(high_t, low) + mm(low_t, high))
    left_scale, left_rest = root_parts(left_gram, ridge, eye)
    right_scale, right_rest = root_parts(right_gram, ridge, eye)
    is_left = owners[block] == index[0]

    @pl.when(is_left)
    def _():
        root_ref[...] = left_scale * (jnp.where(eye, 1.953125, 0.0) - left_rest)

    @pl.when(jnp.logical_not(is_left))
    def _():
        root_ref[...] = right_scale * (jnp.where(eye, 1.953125, 0.0) - right_rest)

    right_product = right_scale * (1.953125 * gradient - mm_split((high, low), halves(right_rest)))
    w_ref[...] = right_product
    l_ref[...] = left_rest
    count = B // piece_rows // 2
    starts = [pl.multiple_of((2 * k + side) * piece_rows, piece_rows) for k in range(count)]
    left_rows = jnp.concatenate([l_ref[pl.ds(s, piece_rows), :] for s in starts], axis=0)
    w_rows = jnp.concatenate([w_ref[pl.ds(s, piece_rows), :] for s in starts], axis=0)
    g_rows = jnp.concatenate([g_ref[pl.ds(s, piece_rows), :] for s in starts], axis=0)
    precond = left_scale * (1.953125 * w_rows - mm_split(halves(left_rows), halves(right_product)))
    p_ref[...] = precond.reshape(count, piece_rows, B)

    def lanes(value):
        total = jnp.sum(value * value, axis=0, keepdims=True)
        return sum(total[:, i : i + 128] for i in range(0, B, 128))

    row_ids = lax.broadcasted_iota(jnp.int32, (8, 128), 0)
    sums_ref[...] = jnp.where(row_ids == 0, lanes(g_rows), jnp.where(row_ids == 1, lanes(precond), 0.0))
    for shift in range(pairs):
        want = (pair + shift) % pairs - block // CB * count
        pieces[shift][...] = p_ref[jnp.clip(want, 0, count - 1)]


def finish_kernel(pairs, piece_rows, index, owners, sums, *refs):
    pieces = refs[:pairs]
    update_ref, graft_ref = refs[pairs:]
    pair = index[0] // 2
    count = B // piece_rows // 2
    grad_total = jnp.sum(sums[0:1, :], keepdims=True)
    precond_total = jnp.sum(sums[1:2, :], keepdims=True)
    graft = jnp.sqrt(grad_total / jnp.maximum(precond_total, 1.0))
    graft_ref[...] = graft
    for c in range(CB):
        source = owners[pair // count * CB + c] // 2
        shift = (pair - source + pairs) % pairs
        for k in range(pairs):

            @pl.when(shift == k)
            def _(k=k, c=c):
                update_ref[:, c * B : (c + 1) * B] = (graft * pieces[k][...]).astype(BF16)


def summed_over(value, axis, bit=1):
    size = lax.axis_size(axis)
    while bit < size:
        value = value + lax.ppermute(value, axis, [(i, i ^ bit) for i in range(size)])
        bit *= 2
    return value


def on_device(activations, cotangents, owners):
    dp_count = lax.axis_size("dp")
    pairs = dp_count // 2
    block_count = owners.shape[0]
    local_tokens, features = activations.shape
    piece_rows = features // dp_count
    mp_count = lax.axis_size("mp")
    parts = mp_count if local_tokens // mp_count >= 16 else 1
    part = lax.axis_index("mp") if parts > 1 else 0
    index = jnp.stack([lax.axis_index("dp"), part]).astype(jnp.int32)
    part_rows = local_tokens // parts
    part_type = jax.ShapeDtypeStruct((part_rows, B), BF16)
    chunk_type = jax.ShapeDtypeStruct((local_tokens, B), BF16)
    packed = pl.pallas_call(
        lambda *refs: pack_kernel(pairs, block_count, *refs),
        out_shape=[part_type] * pairs + [chunk_type] * pairs,
        in_specs=[SMEM, SMEM, VMEM, VMEM],
        out_specs=[VMEM] * (2 * pairs),
    )(index, owners, activations, cotangents)

    def along(value, shift):
        return lax.ppermute(value, "dp", [(i, (i + 2 * shift) % dp_count) for i in range(dp_count)])

    def across(value):
        return lax.ppermute(value, "dp", [(i, i ^ 1) for i in range(dp_count)])

    a_out, c_out = packed[:pairs], packed[pairs:]
    a_mine = jnp.concatenate([a_out[0]] + [along(a_out[s], s) for s in range(1, pairs)], axis=0)
    mine = [c_out[0]]
    own_across = across(c_out[0])
    for s in range(1, pairs):
        mine.append(along(c_out[s], s))
    other = [own_across] + [across(chunk) for chunk in mine[1:]]
    a_other = across(a_mine)
    token_parts = [jnp.concatenate([a_mine, a_other], axis=0)]
    bit = parts // 2
    held = {0: token_parts[0]}
    while bit:
        swap = [(i, i ^ bit) for i in range(mp_count)]
        held.update({m ^ bit: lax.ppermute(v, "mp", swap) for m, v in list(held.items())})
        bit //= 2
    token_parts = [held[m] for m in range(parts)]
    all_tokens = local_tokens * dp_count
    piece_type = jax.ShapeDtypeStruct((piece_rows, B), F32)
    root, sums, *pieces = pl.pallas_call(
        lambda *refs: root_kernel(pairs, parts, block_count, piece_rows, *refs),
        out_shape=[jax.ShapeDtypeStruct((B, B), F32), jax.ShapeDtypeStruct((8, 128), F32)]
        + [piece_type] * pairs,
        in_specs=[SMEM, SMEM] + [VMEM] * (parts + 2 * pairs),
        out_specs=[VMEM] * (pairs + 2),
        scratch_shapes=[
            pltpu.VMEM((all_tokens, B), BF16),
            pltpu.VMEM((all_tokens, B), BF16),
            pltpu.VMEM((B, B), F32),
            pltpu.VMEM((B, B), F32),
            pltpu.VMEM((B, B), F32),
            pltpu.VMEM((B // piece_rows // 2, piece_rows, B), F32),
        ],
    )(index, owners, *token_parts, *mine, *other)
    totals = summed_over(sums, "mp")
    totals = totals + across(totals)
    if pairs <= 4:
        totals = totals + sum(along(totals, s) for s in range(1, pairs))
    else:
        totals = summed_over(totals, "dp", 2)
    arrived = [pieces[0]] + [along(pieces[s], s) for s in range(1, pairs)]
    update, graft = pl.pallas_call(
        lambda *refs: finish_kernel(pairs, piece_rows, *refs),
        out_shape=[
            jax.ShapeDtypeStruct((piece_rows, CB * B), BF16),
            jax.ShapeDtypeStruct((1, 1), F32),
        ],
        in_specs=[SMEM, SMEM] + [VMEM] * (pairs + 1),
        out_specs=[VMEM, VMEM],
    )(index, owners, totals, *arrived)
    return (update, root, graft.reshape(()))


def solution(mesh):
    return jax.shard_map(
        on_device,
        mesh=mesh,
        in_specs=(P("dp", None), P("dp", "mp"), P()),
        out_specs=(P("dp", "mp"), P("dp", "mp"), P()),
        check_vma=False,
    )
```
